32 devices in a mesh: gx: 4 (over x, core), gy: 8 (over z, y).
Axes of the slice: x: 2, y: 2, z: 4, core: 2. Of those that a mesh axis runs over, the one named last changes fastest.
Arguments:
- state: float32 [512, 512, 128], P('gx', 'gy'), may hold values from -6 to 6
- diffusion: float32 [512, 512, 128], P('gx', 'gy'), may hold values from 0.01 to 0.12
- vert_inverse: float32 [512, 128, 128], P('gy'), as said below
- profiles: bfloat16 [8192, 128], P(('gx', 'gy')), may hold values from -6 to 6
- counts: int32 [32, 32], P(('gx', 'gy')), may hold values from 0 to 16, as said below
- cell_lon: int32 [8192], P(('gx', 'gy')), may hold values from 0 to 127
- cell_lat: int32 [8192], P(('gx', 'gy')), may hold values from 0 to 63
- weight_slot: int32 [2, 8192], P(None, ('gx', 'gy')), may hold values from 0 to 63
Outputs:
- adjoint: float32 [512, 512, 128], P('gx', 'gy')
The draws below stay inside these ranges and needn't reach their ends.
Inputs may be any that keep to these rules, and one draw needn't show every extreme that they name: Each row s sums to 256; source device s stores its profiles in order of subdomain, counts[s,d] of them for subdomain d, which covers longitude cells (d // 8) * 128 onwards and latitude cells (d % 8) * 64 onwards. Some subdomain receives 16 profiles from every source. `vert_inverse`: one matrix for each latitude row.
All inputs are finite; a program needn't handle non-finite values.
Results may differ from the reference program's by a relative error of at most 0.0015.
Values may be sent and summed in bfloat16 or wider, within the bound.
A program may use at most 128 MiB of HBM per device.

```python
import math
import jax
import jax.numpy as jnp
from jax import lax

L = 128
CX = 128
CY = 64
CAP = 16
STEPS = 4
SLOTS = 64
NX = 512
NY = 512
OBS = 8192
N_GX = 4
N_GY = 8
DEVICES = 32


def draw_vert_inverse(key, part):
    shape = (NY, L, L)
    noise = jax.random.normal(key, shape, jnp.float32)
    return 0.9 * jnp.eye(L, dtype=jnp.float32)[None] + 0.4 * noise / jnp.sqrt(jnp.float32(L))


def draw_counts(key, part):
    half = CAP // 2
    key_heavy = jax.random.fold_in(key, 11)
    key_rows = jax.random.fold_in(key, 12)
    heavy = jax.random.randint(key_heavy, (), 0, DEVICES)
    ids = jnp.arange(DEVICES, dtype=jnp.int32)

    def one_row(row_key):
        key_perm = jax.random.fold_in(row_key, 1)
        key_amount = jax.random.fold_in(row_key, 2)
        order = jax.random.permutation(key_perm, DEVICES).astype(jnp.int32)
        where_heavy = jnp.sum(jnp.where(order == heavy, ids, 0))
        first = order[0]
        order = order.at[where_heavy].set(first).at[0].set(heavy)
        amount = jax.random.randint(key_amount, (DEVICES // 2,), 0, half + 1).astype(jnp.int32)
        amount = amount.at[0].set(half)
        paired = jnp.stack([amount, -amount], axis=1).reshape(DEVICES)
        change = jnp.zeros((DEVICES,), jnp.int32).at[order].set(paired)
        return half + change
    row_keys = jax.random.split(key_rows, DEVICES)
    return jax.vmap(one_row)(row_keys).astype(jnp.int32)


def place_ends(result, stream_key, low, high):
    place = [jax.random.randint(jax.random.fold_in(stream_key, axis), (), 0, length) for axis, length in enumerate(result.shape)]
    widest = result.shape.index(max(result.shape))
    neighbour = place[:widest] + [(place[widest] + 1) % result.shape[widest]] + place[widest + 1:]
    return result.at[tuple(place)].set(low).at[tuple(neighbour)].set(high)


def block_scale(stream_key, extent, cuts, least, top_value):
    def one(axis_at, shards_of):
        draws = jax.random.uniform(jax.random.fold_in(jax.random.fold_in(stream_key, 6), axis_at), (shards_of,), jnp.float32, least / len(cuts), top_value / len(cuts))
        return jnp.repeat(jnp.exp(draws), extent[axis_at] // shards_of).reshape((-1,) + (1,) * (len(extent) - axis_at - 1))

    level = one(*cuts[0])
    for cut in cuts[1:]:
        level = level * one(*cut)
    return level


def gaussian(rng, dims, width, limit, pieces=(), kind=jnp.bfloat16):
    values = width * jax.random.normal(rng, dims, jnp.float32)
    if pieces:
        values = values * block_scale(rng, dims, pieces, -0.22, 0.18)
    return jnp.clip(values, -limit, limit).astype(kind)


def setup_inputs(seed: int = 0) -> dict:
    streams_of = jax.random.split(jax.random.key(seed), 9)
    state = gaussian(streams_of[0], (NX, NY, L), 1.0, 6.0, ((0, 4), (1, 8)), jnp.float32)
    diffusion = jnp.clip(jnp.exp(math.log(0.12) - 2.4849066 * jax.random.uniform(streams_of[1], (NX, NY, L), jnp.float32) ** block_scale(streams_of[1], (NX, NY, L), ((0, 4), (1, 8)), -0.2, 0.2)), 0.01, 0.12)
    vert_inverse = draw_vert_inverse(jax.random.fold_in(streams_of[8], 71), 0)
    profiles = gaussian(streams_of[3], (OBS, L), 1.0, 6.0, ((0, 32),))
    counts = draw_counts(jax.random.fold_in(streams_of[8], 71), 0)
    cell_lon = place_ends(jax.random.randint(streams_of[5], (OBS,), 0, CX), jax.random.fold_in(streams_of[5], 1), 0, CX - 1).astype(jnp.int32)
    cell_lat = place_ends(jax.random.randint(streams_of[6], (OBS,), 0, CY), jax.random.fold_in(streams_of[6], 1), 0, CY - 1).astype(jnp.int32)
    weight_slot = place_ends(jax.random.randint(streams_of[7], (2, OBS), 0, SLOTS), jax.random.fold_in(streams_of[7], 1), 0, SLOTS - 1).astype(jnp.int32)
    return {"state": state, "diffusion": diffusion, "vert_inverse": vert_inverse, "profiles": profiles, "counts": counts, "cell_lon": cell_lon, "cell_lat": cell_lat, "weight_slot": weight_slot}


def reference(state, diffusion, vert_inverse, profiles, counts, cell_lon, cell_lat, weight_slot):
    devices = N_GX * N_GY
    obs_dev = profiles.shape[0] // devices
    cumulative = jnp.cumsum(counts, axis=1)
    positions = jnp.arange(obs_dev, dtype=jnp.int32)
    owner = jax.vmap(lambda row: jnp.searchsorted(row, positions, side="right"))(cumulative)
    owner = owner.reshape(-1).astype(jnp.int32)
    lon_glob = (owner // N_GY) * CX + cell_lon
    lat_glob = (owner % N_GY) * CY + cell_lat
    frac_x = weight_slot[0].astype(jnp.float32) / SLOTS
    frac_y = weight_slot[1].astype(jnp.float32) / SLOTS
    lon_next = (lon_glob + 1) % NX
    lat_next = lat_glob + 1
    inside = (lat_next < NY).astype(jnp.float32)
    lat_next = jnp.minimum(lat_next, NY - 1)
    targets = jnp.concatenate([lon_glob * NY + lat_glob, lon_next * NY + lat_glob,
                               lon_glob * NY + lat_next, lon_next * NY + lat_next])
    weights = jnp.concatenate([(1.0 - frac_x) * (1.0 - frac_y), frac_x * (1.0 - frac_y),
                               (1.0 - frac_x) * frac_y * inside, frac_x * frac_y * inside])
    values = profiles.astype(jnp.float32)
    terms = weights[:, None] * jnp.concatenate([values, values, values, values])
    forcing = jax.ops.segment_sum(terms, targets, num_segments=NX * NY).reshape(NX, NY, -1)
    lam = state + forcing
    for section in range(STEPS):
        mixed = jnp.einsum("xym,ymk->xyk", lam, vert_inverse, precision=lax.Precision.HIGHEST)
        flux = diffusion * mixed
        padded = jnp.pad(flux, ((0, 0), (1, 1), (0, 0)))
        nearby = jnp.roll(flux, 1, axis=0) + jnp.roll(flux, -1, axis=0) + padded[:, 2:] + padded[:, :-2]
        lam = mixed + nearby - 4.0 * flux
    return lam
```

```python
import functools

import jax
import jax.numpy as jnp
from jax import lax
from jax.experimental import pallas as pl
from jax.experimental.pallas import tpu as pltpu
from jax.sharding import PartitionSpec as P

CAP = 16
STEPS = 4
SLOTS = 64
EDGE = 8
F32 = jnp.float32
BF16 = jnp.bfloat16
MESH = pl.DeviceIdType.MESH
VMEM_LIMIT = 60 * 1024 * 1024


def pack_kernel(prof_ref, counts_ref, lon_ref, lat_ref, slot_ref, out_ref):
    rows_out = out_ref.shape[0]
    obs, levels = prof_ref.shape
    n_dest = counts_ref.shape[1]
    count_row = counts_ref[...].astype(F32)
    dest = lax.broadcasted_iota(jnp.int32, (rows_out, n_dest), 0) // CAP
    lane = lax.broadcasted_iota(jnp.int32, (rows_out, n_dest), 1)
    start = jnp.sum(jnp.where(lane < dest, count_row, 0.0), axis=1, keepdims=True)
    count = jnp.sum(jnp.where(lane == dest, count_row, 0.0), axis=1, keepdims=True)
    slot = (lax.broadcasted_iota(jnp.int32, (rows_out, 1), 0) % CAP).astype(F32)
    source = jnp.where(slot < count, start + slot, -1.0).astype(jnp.int32)
    column = lax.broadcasted_iota(jnp.int32, (rows_out, obs), 1)
    selector = jnp.where(column == source, 1.0, 0.0).astype(BF16)
    kind = lax.broadcasted_iota(jnp.int32, (levels, obs), 0)
    meta = jnp.where(kind == 0, lon_ref[...].astype(F32), 0.0)
    meta = jnp.where(kind == 1, lat_ref[...].astype(F32), meta)
    meta = jnp.where(kind == 2, slot_ref[0:1, :].astype(F32), meta)
    meta = jnp.where(kind == 3, slot_ref[1:2, :].astype(F32), meta)
    out_ref[:, 0:levels] = jnp.dot(
        selector, prof_ref[...], preferred_element_type=F32
    ).astype(BF16)
    out_ref[:, levels:] = lax.dot_general(
        selector, meta.astype(BF16), (((1,), (1,)), ((), ())), preferred_element_type=F32
    ).astype(BF16)


def split(value):
    upper = value.astype(BF16)
    return upper, (value - upper.astype(F32)).astype(BF16)


def step_kernel(
    n_gx, n_gy, group,
    msg_ref, state_hbm, diff_hbm, inv_hbm, out_hbm,
    st, df, wf, wst, mbuf, fbuf, obuf, wx_ref, table, scaled, col_send, col_recv,
    row_send, row_recv, xs, xr, yr,
    in_sem, out_sem, f_send, f_recv, x_send, x_recv, y_send, y_recv,
):
    lat, lon, levels = mbuf.shape
    slots = msg_ref.shape[0]
    gx, gy = lax.axis_index("gx"), lax.axis_index("gy")
    east = (lax.rem(gx + 1, n_gx), gy)
    west = (lax.rem(gx + n_gx - 1, n_gx), gy)
    north = (gx, lax.rem(gy + 1, n_gy))
    south = (gx, lax.rem(gy + n_gy - 1, n_gy))

    loads = [
        pltpu.make_async_copy(src, dst, in_sem.at[i])
        for i, (src, dst) in enumerate(((state_hbm, st), (inv_hbm, wf), (diff_hbm, df)))
    ]
    for load in loads:
        load.start()

    barrier = pltpu.get_barrier_semaphore()
    for peer in (east, west, north, south):
        pl.semaphore_signal(barrier, inc=1, device_id=peer, device_id_type=MESH)

    meta = jnp.transpose(msg_ref[:, levels:].astype(F32))
    lon_row, lat_row = meta[0:1, :], meta[1:2, :]
    frac_x = meta[2:3, :] / SLOTS
    frac_y = msg_ref[:, levels + 3 : levels + 4].astype(F32) / SLOTS
    values = msg_ref[:, 0:levels].astype(F32)
    for half, part in enumerate((values * (1.0 - frac_y), values * frac_y)):
        upper, lower = split(part)
        scaled[half * slots : (half + 1) * slots, 0:levels] = upper
        scaled[half * slots : (half + 1) * slots, levels:] = lower
    x_ids = lax.broadcasted_iota(jnp.int32, (lon, slots), 0).astype(F32)
    wx_ref[...] = jnp.where(x_ids == lon_row, 1.0 - frac_x, 0.0) + jnp.where(
        x_ids == lon_row + 1.0, frac_x, 0.0
    )

    def fold(product):
        return product[:, 0:levels] + product[:, levels:]

    col_rows = col_send.shape[0]
    y_ids = lax.broadcasted_iota(jnp.int32, (col_rows, slots), 0).astype(F32)
    last = jnp.where(lon_row == lon - 1.0, frac_x, 0.0)
    table[0:col_rows, 0:slots] = jnp.where(y_ids == lat_row, last, 0.0).astype(BF16)
    table[0:col_rows, slots:] = jnp.where(y_ids == lat_row + 1.0, last, 0.0).astype(BF16)
    col_send[...] = fold(
        jnp.dot(table[0:col_rows, :], scaled[...], preferred_element_type=F32)
    )
    pl.semaphore_wait(barrier, 4)
    col_copy = pltpu.make_async_remote_copy(
        src_ref=col_send, dst_ref=col_recv, send_sem=f_send.at[0], recv_sem=f_recv.at[0],
        device_id=east, device_id_type=MESH,
    )
    col_copy.start()

    first_x = lax.broadcasted_iota(jnp.int32, (lon, levels), 0) == 0
    table[0:lon, 0:slots] = jnp.zeros((lon, slots), BF16)
    table[0:lon, slots:] = jnp.where(lat_row == lat - 1.0, wx_ref[...], 0.0).astype(BF16)
    over = fold(jnp.dot(table[0:lon, :], scaled[...], preferred_element_type=F32))
    col_copy.wait()
    row_send[...] = over + jnp.where(first_x, col_recv[lat : lat + 1, :], 0.0)
    row_copy = pltpu.make_async_remote_copy(
        src_ref=row_send, dst_ref=row_recv, send_sem=f_send.at[1], recv_sem=f_recv.at[1],
        device_id=north, device_id_type=MESH,
    )
    row_copy.start()

    def force(index, carry):
        for j in range(group):
            here = (index * group + j).astype(F32)
            rows = slice(j * lon, (j + 1) * lon)
            table[rows, 0:slots] = jnp.where(lat_row == here, wx_ref[...], 0.0).astype(BF16)
            table[rows, slots:] = jnp.where(lat_row + 1.0 == here, wx_ref[...], 0.0).astype(BF16)
        total = fold(jnp.dot(table[...], scaled[...], preferred_element_type=F32))
        for j in range(group):
            y = index * group + j
            mbuf[y] = total[j * lon : (j + 1) * lon] + jnp.where(
                first_x, col_recv[pl.ds(y, 1), :], 0.0
            )
        return carry

    lax.fori_loop(0, lat // group, force, 0)
    row_copy.wait()
    mbuf[0] = mbuf[0] + jnp.where(gy > 0, row_recv[...], 0.0)

    middle = (lat // 2) // EDGE * EDGE
    chunks = ((0, EDGE), (lat - EDGE, lat), (EDGE, middle), (middle, lat - EDGE))
    last_x = lax.broadcasted_iota(jnp.int32, (lon, levels), 0) == lon - 1

    def x_copies(step, chunk):
        low, high = chunks[chunk]
        copies = []
        for side, peer in ((0, west), (1, east)):
            k = (step * 2 + side) * len(chunks) + chunk
            copies.append(
                pltpu.make_async_remote_copy(
                    src_ref=xs.at[step % 2, side, pl.ds(low, high - low)],
                    dst_ref=xr.at[step, 1 - side, pl.ds(low, high - low)],
                    send_sem=x_send.at[k], recv_sem=x_recv.at[k],
                    device_id=peer, device_id_type=MESH,
                )
            )
        return copies

    def y_copies(step):
        copies = []
        for side, peer in ((0, south), (1, north)):
            k = step * 2 + side
            copies.append(
                pltpu.make_async_remote_copy(
                    src_ref=fbuf.at[step % 2, lat if side else 1],
                    dst_ref=yr.at[step, 1 - side],
                    send_sem=y_send.at[k], recv_sem=y_recv.at[k],
                    device_id=peer, device_id_type=MESH,
                )
            )
        return copies

    def advanced(step, y):
        old = step % 2
        centre = fbuf[old, y + 1]
        behind = jnp.where(first_x, xr[step, 0, pl.ds(y, 1), :], pltpu.roll(centre, 1, 0))
        ahead = jnp.where(last_x, xr[step, 1, pl.ds(y, 1), :], pltpu.roll(centre, lon - 1, 0))
        return mbuf[y] + ((behind + ahead) + (fbuf[old, y] + fbuf[old, y + 2]))

    def section(step, y):
        if step == 0:
            lam = st[pl.ds(y, lon, stride=lat), :] + mbuf[y]
            pair = jnp.concatenate(split(wf[y]), axis=1)
            wst[y] = pair
        else:
            lam = advanced(step - 1, y)
            pair = wst[y]
        mixed = fold(
            jnp.dot(
                jnp.concatenate(split(lam), axis=1),
                jnp.concatenate([pair, pair], axis=0),
                preferred_element_type=F32,
            )
        )
        flux = df[pl.ds(y, lon, stride=lat), :] * mixed
        mbuf[y] = mixed - 4.0 * flux
        fbuf[step % 2, y + 1] = flux
        xs[step % 2, 0, pl.ds(y, 1), :] = flux[0:1]
        xs[step % 2, 1, pl.ds(y, 1), :] = flux[lon - 1 : lon]

    def sweep(work, low, high):
        def two(index, carry):
            work(low + 2 * index)
            work(low + 2 * index + 1)
            return carry

        lax.fori_loop(0, (high - low) // 2, two, 0)

    def halo(step):
        for copy in y_copies(step):
            copy.wait()
        fbuf[step % 2, 0] = jnp.where(gy > 0, yr[step, 0], 0.0)
        fbuf[step % 2, lat + 1] = jnp.where(gy < n_gy - 1, yr[step, 1], 0.0)

    for load in loads:
        load.wait()
    for step in range(STEPS):
        if step:
            halo(step - 1)
        for chunk, (low, high) in enumerate(chunks):
            if step:
                for copy in x_copies(step - 1, chunk):
                    copy.wait()
            sweep(functools.partial(section, step), low, high)
            if chunk == 1:
                for copy in y_copies(step):
                    copy.start()
            for copy in x_copies(step, chunk):
                copy.start()

    def finish(y):
        obuf[y] = advanced(STEPS - 1, y)

    halo(STEPS - 1)
    stores = []
    for chunk, (low, high) in enumerate(chunks):
        for copy in x_copies(STEPS - 1, chunk):
            copy.wait()
        sweep(finish, low, high)
        part = pl.ds(low, high - low)
        stores.append(pltpu.make_async_copy(obuf.at[part], out_hbm.at[part], out_sem.at[chunk]))
        stores[-1].start()
    for store in stores:
        store.wait()


def solution(mesh):
    n_gx, n_gy = mesh.shape["gx"], mesh.shape["gy"]

    def shards(state, diffusion, vert_inverse, profiles, counts, cell_lon, cell_lat, weight_slot):
        lon, lat, levels = state.shape
        n_dest = counts.shape[1]
        slots = n_dest * CAP
        group = 4
        message = pl.pallas_call(
            pack_kernel,
            out_shape=jax.ShapeDtypeStruct((slots, 2 * levels), BF16),
            compiler_params=pltpu.CompilerParams(vmem_limit_bytes=VMEM_LIMIT),
            name="pack",
        )(profiles, counts, cell_lon[None], cell_lat[None], weight_slot)
        message = lax.all_to_all(
            message.reshape(n_dest, CAP, 2 * levels), ("gx", "gy"),
            split_axis=0, concat_axis=0, tiled=True,
        ).reshape(slots, 2 * levels)
        n_x = STEPS * 2 * 4
        dma = pltpu.SemaphoreType.DMA
        out = pl.pallas_call(
            functools.partial(step_kernel, n_gx, n_gy, group),
            out_shape=jax.ShapeDtypeStruct((lat, lon, levels), F32),
            in_specs=[pl.BlockSpec(memory_space=pltpu.VMEM)]
            + [pl.BlockSpec(memory_space=pl.ANY)] * 3,
            out_specs=pl.BlockSpec(memory_space=pl.ANY),
            scratch_shapes=[
                pltpu.VMEM((lon * lat, levels), F32),
                pltpu.VMEM((lon * lat, levels), F32),
                pltpu.VMEM((lat, levels, levels), F32),
                pltpu.VMEM((lat, levels, 2 * levels), BF16),
                pltpu.VMEM((lat, lon, levels), F32),
                pltpu.VMEM((2, lat + 2, lon, levels), F32),
                pltpu.VMEM((lat, lon, levels), F32),
                pltpu.VMEM((lon, slots), F32),
                pltpu.VMEM((group * lon, 2 * slots), BF16),
                pltpu.VMEM((2 * slots, 2 * levels), BF16),
                pltpu.VMEM((lat + 8, levels), F32),
                pltpu.VMEM((lat + 8, levels), F32),
                pltpu.VMEM((lon, levels), F32),
                pltpu.VMEM((lon, levels), F32),
                pltpu.VMEM((2, 2, lat, levels), F32),
                pltpu.VMEM((STEPS, 2, lat, levels), F32),
                pltpu.VMEM((STEPS, 2, lon, levels), F32),
                dma((3,)), dma((4,)), dma((2,)), dma((2,)),
                dma((n_x,)), dma((n_x,)), dma((STEPS * 2,)), dma((STEPS * 2,)),
            ],
            compiler_params=pltpu.CompilerParams(
                collective_id=0, has_side_effects=True, vmem_limit_bytes=VMEM_LIMIT
            ),
            name="steps",
        )(
            message,
            state.reshape(lon * lat, levels),
            diffusion.reshape(lon * lat, levels),
            vert_inverse,
        )
        return jnp.transpose(out, (1, 0, 2))

    return jax.shard_map(
        shards,
        mesh=mesh,
        in_specs=(
            P("gx", "gy", None),
            P("gx", "gy", None),
            P("gy", None, None),
            P(("gx", "gy"), None),
            P(("gx", "gy"), None),
            P(("gx", "gy")),
            P(("gx", "gy")),
            P(None, ("gx", "gy")),
        ),
        out_specs=P("gx", "gy", None),
        check_vma=False,
    )
```

```python
import functools

import jax
import jax.numpy as jnp
from jax import lax
from jax.experimental import pallas as pl
from jax.experimental.pallas import tpu as pltpu
from jax.sharding import PartitionSpec as P

CAP = 16
STEPS = 4
SLOTS = 64
EDGE = 8
F32 = jnp.float32
BF16 = jnp.bfloat16
MESH = pl.DeviceIdType.MESH
VMEM_LIMIT = 60 * 1024 * 1024


def pack_kernel(
    n_gy, prof_ref, counts_ref, lon_ref, lat_ref, slot_ref, out_ref, msg, recv, send_sem, recv_sem
):
    n_all = msg.shape[0]
    me = lax.axis_index("gx") * n_gy + lax.axis_index("gy")

    def peer(offset):
        other = lax.rem(me + offset, n_all)
        return other, (other // n_gy, lax.rem(other, n_gy))

    barrier = pltpu.get_barrier_semaphore()

    def greet(offset, carry):
        pl.semaphore_signal(barrier, inc=1, device_id=peer(offset)[1], device_id_type=MESH)
        return carry

    lax.fori_loop(1, n_all, greet, 0)
    rows_out = n_all * CAP
    obs, levels = prof_ref.shape
    n_dest = counts_ref.shape[1]
    count_row = counts_ref[...].astype(F32)
    dest = lax.broadcasted_iota(jnp.int32, (rows_out, n_dest), 0) // CAP
    lane = lax.broadcasted_iota(jnp.int32, (rows_out, n_dest), 1)
    start = jnp.sum(jnp.where(lane < dest, count_row, 0.0), axis=1, keepdims=True)
    count = jnp.sum(jnp.where(lane == dest, count_row, 0.0), axis=1, keepdims=True)
    slot = (lax.broadcasted_iota(jnp.int32, (rows_out, 1), 0) % CAP).astype(F32)
    source = jnp.where(slot < count, start + slot, -1.0).astype(jnp.int32)
    column = lax.broadcasted_iota(jnp.int32, (rows_out, obs), 1)
    selector = jnp.where(column == source, 1.0, 0.0).astype(BF16)
    kind = lax.broadcasted_iota(jnp.int32, (levels, obs), 0)
    meta = jnp.where(kind == 0, lon_ref[...].astype(F32), 0.0)
    meta = jnp.where(kind == 1, lat_ref[...].astype(F32), meta)
    meta = jnp.where(kind == 2, slot_ref[0:1, :].astype(F32), meta)
    meta = jnp.where(kind == 3, slot_ref[1:2, :].astype(F32), meta)
    msg[:, :, 0:levels] = (
        jnp.dot(selector, prof_ref[...], preferred_element_type=F32)
        .astype(BF16)
        .reshape(n_all, CAP, levels)
    )
    msg[:, :, levels:] = (
        lax.dot_general(
            selector, meta.astype(BF16), (((1,), (1,)), ((), ())), preferred_element_type=F32
        )
        .astype(BF16)
        .reshape(n_all, CAP, levels)
    )
    pl.semaphore_wait(barrier, n_all - 1)

    def block_copy(offset):
        other, device = peer(offset)
        return pltpu.make_async_remote_copy(
            src_ref=msg.at[other], dst_ref=recv.at[me],
            send_sem=send_sem.at[offset], recv_sem=recv_sem.at[offset],
            device_id=device, device_id_type=MESH,
        )

    def send(offset, carry):
        block_copy(offset).start()
        return carry

    def arrive(offset, carry):
        block_copy(offset).wait()
        return carry

    lax.fori_loop(1, n_all, send, 0)
    recv[me] = msg[me]
    lax.fori_loop(1, n_all, arrive, 0)
    out_ref[...] = recv[...]


def split(value):
    upper = value.astype(BF16)
    return upper, (value - upper.astype(F32)).astype(BF16)


def step_kernel(
    n_gx, n_gy, group,
    msg_ref, state_hbm, diff_hbm, inv_hbm, out_hbm,
    st, df, wf, wst, mbuf, fbuf, obuf, wx_ref, table, scaled, col_send, col_recv,
    row_send, row_recv, xs, xr, yr,
    in_sem, out_sem, f_send, f_recv, x_send, x_recv, y_send, y_recv,
):
    lat, lon, levels = mbuf.shape
    slots = msg_ref.shape[0]
    gx, gy = lax.axis_index("gx"), lax.axis_index("gy")
    east = (lax.rem(gx + 1, n_gx), gy)
    west = (lax.rem(gx + n_gx - 1, n_gx), gy)
    north = (gx, lax.rem(gy + 1, n_gy))
    south = (gx, lax.rem(gy + n_gy - 1, n_gy))

    loads = [
        pltpu.make_async_copy(src, dst, in_sem.at[i])
        for i, (src, dst) in enumerate(((state_hbm, st), (inv_hbm, wf), (diff_hbm, df)))
    ]
    for load in loads:
        load.start()

    barrier = pltpu.get_barrier_semaphore()
    for peer in (east, west, north, south):
        pl.semaphore_signal(barrier, inc=1, device_id=peer, device_id_type=MESH)

    meta = jnp.transpose(msg_ref[:, levels:].astype(F32))
    lon_row, lat_row = meta[0:1, :], meta[1:2, :]
    frac_x = meta[2:3, :] / SLOTS
    frac_y = msg_ref[:, levels + 3 : levels + 4].astype(F32) / SLOTS
    values = msg_ref[:, 0:levels].astype(F32)
    for half, part in enumerate((values * (1.0 - frac_y), values * frac_y)):
        upper, lower = split(part)
        scaled[half * slots : (half + 1) * slots, 0:levels] = upper
        scaled[half * slots : (half + 1) * slots, levels:] = lower
    x_ids = lax.broadcasted_iota(jnp.int32, (lon, slots), 0).astype(F32)
    wx_ref[...] = jnp.where(x_ids == lon_row, 1.0 - frac_x, 0.0) + jnp.where(
        x_ids == lon_row + 1.0, frac_x, 0.0
    )

    def fold(product):
        return product[:, 0:levels] + product[:, levels:]

    col_rows = col_send.shape[0]
    y_ids = lax.broadcasted_iota(jnp.int32, (col_rows, slots), 0).astype(F32)
    last = jnp.where(lon_row == lon - 1.0, frac_x, 0.0)
    table[0:col_rows, 0:slots] = jnp.where(y_ids == lat_row, last, 0.0).astype(BF16)
    table[0:col_rows, slots:] = jnp.where(y_ids == lat_row + 1.0, last, 0.0).astype(BF16)
    col_send[...] = fold(
        jnp.dot(table[0:col_rows, :], scaled[...], preferred_element_type=F32)
    )
    pl.semaphore_wait(barrier, 4)
    col_copy = pltpu.make_async_remote_copy(
        src_ref=col_send, dst_ref=col_recv, send_sem=f_send.at[0], recv_sem=f_recv.at[0],
        device_id=east, device_id_type=MESH,
    )
    col_copy.start()

    first_x = lax.broadcasted_iota(jnp.int32, (lon, levels), 0) == 0
    table[0:lon, 0:slots] = jnp.zeros((lon, slots), BF16)
    table[0:lon, slots:] = jnp.where(lat_row == lat - 1.0, wx_ref[...], 0.0).astype(BF16)
    over = fold(jnp.dot(table[0:lon, :], scaled[...], preferred_element_type=F32))
    col_copy.wait()
    row_send[...] = over + jnp.where(first_x, col_recv[lat : lat + 1, :], 0.0)
    row_copy = pltpu.make_async_remote_copy(
        src_ref=row_send, dst_ref=row_recv, send_sem=f_send.at[1], recv_sem=f_recv.at[1],
        device_id=north, device_id_type=MESH,
    )
    row_copy.start()

    def force(index, carry):
        for j in range(group):
            here = (index * group + j).astype(F32)
            rows = slice(j * lon, (j + 1) * lon)
            table[rows, 0:slots] = jnp.where(lat_row == here, wx_ref[...], 0.0).astype(BF16)
            table[rows, slots:] = jnp.where(lat_row + 1.0 == here, wx_ref[...], 0.0).astype(BF16)
        total = fold(jnp.dot(table[...], scaled[...], preferred_element_type=F32))
        for j in range(group):
            y = index * group + j
            mbuf[y] = total[j * lon : (j + 1) * lon] + jnp.where(
                first_x, col_recv[pl.ds(y, 1), :], 0.0
            )
        return carry

    lax.fori_loop(0, lat // group, force, 0)
    row_copy.wait()
    mbuf[0] = mbuf[0] + jnp.where(gy > 0, row_recv[...], 0.0)

    middle = (lat // 2) // EDGE * EDGE
    chunks = ((0, EDGE), (lat - EDGE, lat), (EDGE, middle), (middle, lat - EDGE))
    last_x = lax.broadcasted_iota(jnp.int32, (lon, levels), 0) == lon - 1

    def x_copies(step, chunk):
        low, high = chunks[chunk]
        copies = []
        for side, peer in ((0, west), (1, east)):
            k = (step * 2 + side) * len(chunks) + chunk
            copies.append(
                pltpu.make_async_remote_copy(
                    src_ref=xs.at[step % 2, side, pl.ds(low, high - low)],
                    dst_ref=xr.at[step, 1 - side, pl.ds(low, high - low)],
                    send_sem=x_send.at[k], recv_sem=x_recv.at[k],
                    device_id=peer, device_id_type=MESH,
                )
            )
        return copies

    def y_copies(step):
        copies = []
        for side, peer in ((0, south), (1, north)):
            k = step * 2 + side
            copies.append(
                pltpu.make_async_remote_copy(
                    src_ref=fbuf.at[step % 2, lat if side else 1],
                    dst_ref=yr.at[step, 1 - side],
                    send_sem=y_send.at[k], recv_sem=y_recv.at[k],
                    device_id=peer, device_id_type=MESH,
                )
            )
        return copies

    def advanced(step, y):
        old = step % 2
        centre = fbuf[old, y + 1]
        behind = jnp.where(first_x, xr[step, 0, pl.ds(y, 1), :], pltpu.roll(centre, 1, 0))
        ahead = jnp.where(last_x, xr[step, 1, pl.ds(y, 1), :], pltpu.roll(centre, lon - 1, 0))
        return mbuf[y] + ((behind + ahead) + (fbuf[old, y] + fbuf[old, y + 2]))

    def section(step, y):
        if step == 0:
            lam = st[pl.ds(y, lon, stride=lat), :] + mbuf[y]
            pair = jnp.concatenate(split(wf[y]), axis=1)
            wst[y] = pair
        else:
            lam = advanced(step - 1, y)
            pair = wst[y]
        mixed = fold(
            jnp.dot(
                jnp.concatenate(split(lam), axis=1),
                jnp.concatenate([pair, pair], axis=0),
                preferred_element_type=F32,
            )
        )
        flux = df[pl.ds(y, lon, stride=lat), :] * mixed
        mbuf[y] = mixed - 4.0 * flux
        fbuf[step % 2, y + 1] = flux
        xs[step % 2, 0, pl.ds(y, 1), :] = flux[0:1]
        xs[step % 2, 1, pl.ds(y, 1), :] = flux[lon - 1 : lon]

    def sweep(work, low, high):
        def two(index, carry):
            work(low + 2 * index)
            work(low + 2 * index + 1)
            return carry

        lax.fori_loop(0, (high - low) // 2, two, 0)

    def halo(step):
        for copy in y_copies(step):
            copy.wait()
        fbuf[step % 2, 0] = jnp.where(gy > 0, yr[step, 0], 0.0)
        fbuf[step % 2, lat + 1] = jnp.where(gy < n_gy - 1, yr[step, 1], 0.0)

    for load in loads:
        load.wait()
    for step in range(STEPS):
        if step:
            halo(step - 1)
        for chunk, (low, high) in enumerate(chunks):
            if step:
                for copy in x_copies(step - 1, chunk):
                    copy.wait()
            sweep(functools.partial(section, step), low, high)
            if chunk == 1:
                for copy in y_copies(step):
                    copy.start()
            for copy in x_copies(step, chunk):
                copy.start()

    def finish(y):
        obuf[y] = advanced(STEPS - 1, y)

    halo(STEPS - 1)
    stores = []
    for chunk, (low, high) in enumerate(chunks):
        for copy in x_copies(STEPS - 1, chunk):
            copy.wait()
        sweep(finish, low, high)
        part = pl.ds(low, high - low)
        stores.append(pltpu.make_async_copy(obuf.at[part], out_hbm.at[part], out_sem.at[chunk]))
        stores[-1].start()
    for store in stores:
        store.wait()


def solution(mesh):
    n_gx, n_gy = mesh.shape["gx"], mesh.shape["gy"]

    def shards(state, diffusion, vert_inverse, profiles, counts, cell_lon, cell_lat, weight_slot):
        lon, lat, levels = state.shape
        n_dest = counts.shape[1]
        slots = n_dest * CAP
        group = 4
        block = (n_dest, CAP, 2 * levels)
        message = pl.pallas_call(
            functools.partial(pack_kernel, n_gy),
            out_shape=jax.ShapeDtypeStruct(block, BF16),
            scratch_shapes=[
                pltpu.VMEM(block, BF16),
                pltpu.VMEM(block, BF16),
                pltpu.SemaphoreType.DMA((n_dest,)),
                pltpu.SemaphoreType.DMA((n_dest,)),
            ],
            compiler_params=pltpu.CompilerParams(
                collective_id=1, has_side_effects=True, vmem_limit_bytes=VMEM_LIMIT
            ),
            name="pack",
        )(profiles, counts, cell_lon[None], cell_lat[None], weight_slot)
        message = message.reshape(slots, 2 * levels)
        n_x = STEPS * 2 * 4
        dma = pltpu.SemaphoreType.DMA
        out = pl.pallas_call(
            functools.partial(step_kernel, n_gx, n_gy, group),
            out_shape=jax.ShapeDtypeStruct((lat, lon, levels), F32),
            in_specs=[pl.BlockSpec(memory_space=pltpu.VMEM)]
            + [pl.BlockSpec(memory_space=pl.ANY)] * 3,
            out_specs=pl.BlockSpec(memory_space=pl.ANY),
            scratch_shapes=[
                pltpu.VMEM((lon * lat, levels), F32),
                pltpu.VMEM((lon * lat, levels), F32),
                pltpu.VMEM((lat, levels, levels), F32),
                pltpu.VMEM((lat, levels, 2 * levels), BF16),
                pltpu.VMEM((lat, lon, levels), F32),
                pltpu.VMEM((2, lat + 2, lon, levels), F32),
                pltpu.VMEM((lat, lon, levels), F32),
                pltpu.VMEM((lon, slots), F32),
                pltpu.VMEM((group * lon, 2 * slots), BF16),
                pltpu.VMEM((2 * slots, 2 * levels), BF16),
                pltpu.VMEM((lat + 8, levels), F32),
                pltpu.VMEM((lat + 8, levels), F32),
                pltpu.VMEM((lon, levels), F32),
                pltpu.VMEM((lon, levels), F32),
                pltpu.VMEM((2, 2, lat, levels), F32),
                pltpu.VMEM((STEPS, 2, lat, levels), F32),
                pltpu.VMEM((STEPS, 2, lon, levels), F32),
                dma((3,)), dma((4,)), dma((2,)), dma((2,)),
                dma((n_x,)), dma((n_x,)), dma((STEPS * 2,)), dma((STEPS * 2,)),
            ],
            compiler_params=pltpu.CompilerParams(
                collective_id=0, has_side_effects=True, vmem_limit_bytes=VMEM_LIMIT
            ),
            name="steps",
        )(
            message,
            state.reshape(lon * lat, levels),
            diffusion.reshape(lon * lat, levels),
            vert_inverse,
        )
        return jnp.transpose(out, (1, 0, 2))

    return jax.shard_map(
        shards,
        mesh=mesh,
        in_specs=(
            P("gx", "gy", None),
            P("gx", "gy", None),
            P("gy", None, None),
            P(("gx", "gy"), None),
            P(("gx", "gy"), None),
            P(("gx", "gy")),
            P(("gx", "gy")),
            P(None, ("gx", "gy")),
        ),
        out_specs=P("gx", "gy", None),
        check_vma=False,
    )
```
